256 devices in a mesh: prow: 16 (over z, core), pcol: 16 (over x, y).
Axes of the slice: x: 4, y: 4, z: 8, core: 2. Of those that a mesh axis runs over, the one named last changes fastest.
Arguments:
- inv_lead: float32 [4, 16, 256, 4, 16, 256], P(None, 'prow', None, None, 'pcol'), may hold values from -1 to 2, as said below
- h_lead: float32 [4, 16, 256, 6, 16, 256], P(None, 'pcol', None, None, 'prow'), may hold values from -6 to 6
- h_slab: float32 [512, 6, 16, 256], P('pcol', None, 'prow'), may hold values from -6 to 6
- l_panel: float32 [512, 4, 16, 256], P('pcol', None, 'prow'), may hold values from -0.046875 to 0.046875
- l_diag: float32 [512, 512], replicated, may hold values from -1 to 2, as said below
Outputs:
- x_slab: float32 [512, 6, 16, 256], P('pcol', None, 'prow')
- y_lead: float32 [512, 4, 16, 256], P('pcol', None, 'prow')
- y_diag: float32 [512, 512], P('pcol', 'prow')
The draws below stay inside these ranges and needn't reach their ends.
Inputs may be any that keep to these rules, and one draw needn't show every extreme that they name: inv_lead is lower triangular in natural order, with diagonal entries between 1 and 2. l_diag is lower triangular, with diagonal entries between 1 and 2.
All inputs are finite; a program needn't handle non-finite values.
Results may differ from the reference program's by a relative error of at most 0.00018.
Values sent between devices are 32-bit elements; how exact they have to be, the bound alone decides.
No kernel may reach another device: no remote copies, remote signals or barrier semaphores. Data moves between devices by JAX's collectives and lax.ppermute only.
A program may use at most 128 MiB of HBM per device.

```python
import jax
import jax.numpy as jnp
from jax import lax

NB = 256
SLAB = 512
N = 24576
KBD = 4
KB = 64
KR = 16384
CBD = 4
NCP = 6
N_PROW = 16
N_PCOL = 16


def draw_inv_lead(key, part):
    first_key, second_key = jax.random.split(jax.random.fold_in(key, 11))
    off_diag = jax.random.normal(first_key, (KR, KR), jnp.float32) / jnp.sqrt(jnp.float32(KR))
    diagonal = jax.random.uniform(second_key, (KR,), jnp.float32, 1.0, 2.0)
    matrix = jnp.tril(off_diag, -1) + jnp.diag(diagonal)
    return matrix.reshape(KBD, KB // KBD, NB, CBD, KB // CBD, NB)


def draw_l_diag(key, part):
    first_key, second_key = jax.random.split(jax.random.fold_in(key, 23))
    off_diag = jax.random.normal(first_key, (SLAB, SLAB), jnp.float32) / jnp.sqrt(jnp.float32(SLAB))
    diagonal = jax.random.uniform(second_key, (SLAB,), jnp.float32, 1.0, 2.0)
    return jnp.tril(off_diag, -1) + jnp.diag(diagonal)


def levels(key, extent, cuts, least, high):
    factor_of = 1.0
    for axis_at, blocks in cuts:
        draws = jax.random.uniform(jax.random.fold_in(jax.random.fold_in(key, 6), axis_at), (blocks,), jnp.float32, least / len(cuts), high / len(cuts))
        factor_of = factor_of * jnp.repeat(jnp.exp(draws), extent[axis_at] // blocks).reshape((-1,) + (1,) * (len(extent) - 1 - axis_at))
    return factor_of


def bell_draw(own_key, extent, width, most, cuts=(), kind=jnp.bfloat16):
    level = levels(own_key, extent, cuts, -0.22, 0.18) if cuts else 1.0
    values = jax.random.normal(own_key, extent, jnp.float32) * width * level
    return jnp.minimum(jnp.maximum(values, -most), most).astype(kind)


def setup_inputs(seed: int = 0) -> dict:
    seeds = jax.random.split(jax.random.key(seed), 6)
    inv_lead = draw_inv_lead(jax.random.fold_in(seeds[5], 71), 0)
    h_lead = bell_draw(seeds[1], (CBD, N_PCOL, NB, NCP, N_PROW, NB), 1.0, 6.0, ((1, 16), (4, 16)), jnp.float32)
    h_slab = bell_draw(seeds[2], (SLAB, NCP, N_PROW, NB), 1.0, 6.0, ((0, 16), (2, 16)), jnp.float32)
    l_panel = bell_draw(seeds[3], (SLAB, KBD, N_PROW, NB), KR ** -0.5, 0.046875, ((0, 16), (2, 16)), jnp.float32)
    l_diag = draw_l_diag(jax.random.fold_in(seeds[5], 71), 0)
    return {"inv_lead": inv_lead, "h_lead": h_lead, "h_slab": h_slab, "l_panel": l_panel, "l_diag": l_diag}


def matmul_hi(left, right):
    return jnp.dot(left.astype(jnp.float32), right.astype(jnp.float32), precision=lax.Precision.HIGHEST, preferred_element_type=jnp.float32)

def invert_diag(l_diag, block_size):
    diag_top = l_diag[:block_size, :block_size]
    diag_bottom = l_diag[block_size:, block_size:]
    off_block = l_diag[block_size:, :block_size]
    identity = jnp.eye(block_size, dtype=jnp.float32)
    top_inv = lax.linalg.triangular_solve(diag_top, identity, left_side=True, lower=True)
    bottom_inv = lax.linalg.triangular_solve(diag_bottom, identity, left_side=True, lower=True)
    corner = -matmul_hi(bottom_inv, matmul_hi(off_block, top_inv))
    upper_rows = jnp.concatenate([top_inv, jnp.zeros_like(top_inv)], axis=1)
    lower_rows = jnp.concatenate([corner, bottom_inv], axis=1)
    return jnp.concatenate([upper_rows, lower_rows], axis=0)

def reference(inv_lead, h_lead, h_slab, l_panel, l_diag):
    inv_full = inv_lead.reshape(KR, KR)
    h_first = h_lead.reshape(KR, N)
    h_side = h_slab.reshape(SLAB, N)
    l_rows = l_panel.reshape(SLAB, KR)
    diag_inv = invert_diag(l_diag, NB)
    factor = matmul_hi(diag_inv, l_rows)
    inv_panel = -matmul_hi(factor, inv_full)
    x_full = matmul_hi(inv_panel, h_first) + matmul_hi(diag_inv, h_side)
    head_cols = x_full[:, :KR]
    tail_cols = x_full[:, KR:KR + SLAB]
    y_first = matmul_hi(head_cols, inv_full.T)
    y_block = matmul_hi(head_cols, inv_panel.T) + matmul_hi(tail_cols, diag_inv.T)
    return (x_full.reshape(SLAB, NCP, N_PROW, NB), y_first.reshape(SLAB, KBD, N_PROW, NB), y_block)
```

```python
import functools

import jax
import jax.numpy as jnp
from jax import lax
from jax.experimental import pallas as pl
from jax.experimental.pallas import tpu as pltpu
from jax.sharding import Mesh, PartitionSpec as P

AXES = ("z", "core", "x", "y")
PROW = ("z", "core")
PCOL = ("x", "y")
HIGH = lax.Precision.HIGH
HIGHEST = lax.Precision.HIGHEST


def dot(left, right, contract, precision=HIGH):
    return lax.dot_general(left, right, (contract, ((), ())), precision=precision, preferred_element_type=jnp.float32)


def rows_kernel(tiles, rows, flat_ref, out_ref):
    for tile in range(tiles):
        out_ref[:, tile * 128 : (tile + 1) * 128] = flat_ref[pl.ds(tile, rows, stride=tiles), :]


def as_matrix(block, rows, step=256):
    tiles = block.size // rows // 128
    return pl.pallas_call(
        functools.partial(rows_kernel, tiles, step),
        grid=(rows // step,),
        in_specs=[pl.BlockSpec((step * tiles, 128), lambda i: (i, 0))],
        out_specs=pl.BlockSpec((step, tiles * 128), lambda i: (i, 0)),
        out_shape=jax.ShapeDtypeStruct((rows, tiles * 128), jnp.float32),
        cost_estimate=pl.CostEstimate(flops=0, bytes_accessed=8 * block.size, transcendentals=0),
        name="as_matrix",
    )(block.reshape(rows * tiles, 128))


def invert_kernel(half, l_ref, out_ref):
    rows = lax.broadcasted_iota(jnp.int32, (half, half), 0)
    cols = lax.broadcasted_iota(jnp.int32, (half, half), 1)
    on_diag = rows == cols
    mm = functools.partial(dot, contract=((1,), (0,)), precision=HIGHEST)
    blocks = [l_ref[k * half : (k + 1) * half, k * half : (k + 1) * half] for k in range(2)]
    inverses = [jnp.where(on_diag, 1.0 / jnp.where(on_diag, block, 1.0), 0.0) for block in blocks]
    size = 1
    while size < half:
        row_block, col_block = rows // size, cols // size
        below = (row_block == col_block + 1) & (row_block % 2 == 1)
        offs = [jnp.where(below, block, 0.0) for block in blocks]
        halves = [mm(off, inverse) for off, inverse in zip(offs, inverses)]
        inverses = [inverse - mm(inverse, term) for inverse, term in zip(inverses, halves)]
        size *= 2
    corner = mm(inverses[1], mm(l_ref[half:, :half], inverses[0]))
    out_ref[:half, :half] = inverses[0]
    out_ref[:half, half:] = jnp.zeros((half, half), jnp.float32)
    out_ref[half:, :half] = -corner
    out_ref[half:, half:] = inverses[1]


def invert_diag(l_diag):
    size = l_diag.shape[0]
    return pl.pallas_call(
        functools.partial(invert_kernel, size // 2),
        out_shape=jax.ShapeDtypeStruct(l_diag.shape, jnp.float32),
        cost_estimate=pl.CostEstimate(flops=40 * size**3, bytes_accessed=8 * size * size, transcendentals=0),
        name="invert_diag",
    )(l_diag)


def exchange(value, axis):
    return lax.all_to_all(value, axis, split_axis=0, concat_axis=0, tiled=True)


def per_device(inv_lead, h_lead, h_slab, l_panel, l_diag):
    slab = l_diag.shape[0]
    n_blocks, nb = l_panel.shape[1], l_panel.shape[3]
    h_blocks = h_slab.shape[1]
    x_rows = l_panel.shape[0]
    n_z, n_core = lax.axis_size("z"), lax.axis_size("core")
    n_row = n_z * n_core
    n_col = lax.axis_size("x") * lax.axis_size("y")
    core = lax.axis_index("core")
    row = lax.axis_index(PROW)
    col = lax.axis_index(PCOL)
    width = n_blocks * nb
    lead_at = width // n_row
    y_rows = slab // n_row

    own_p = l_panel.reshape(x_rows, width)
    p_rows = exchange(jnp.broadcast_to(own_p, (n_col, *own_p.shape)), PCOL).reshape(slab, width)

    dinv = invert_diag(l_diag)
    m_local = as_matrix(inv_lead, width)
    h_local = as_matrix(h_lead, width)
    h_side = h_slab.reshape(x_rows, h_blocks * nb)

    partial = dot(m_local, p_rows, ((0,), (1,)))
    pieces = partial.reshape(n_z, n_core, lead_at, slab)
    kept = lax.dynamic_index_in_dim(pieces, core, 1, keepdims=False)
    sent = lax.dynamic_index_in_dim(pieces, 1 - core, 1, keepdims=False)
    swap = [(0, 1), (1, 0)]
    pair = kept + lax.ppermute(sent, "core", swap)
    own_sum = exchange(pair, "z").sum(axis=0)
    own_panel = -dot(own_sum, dinv, ((1,), (1,)))
    panel_t = lax.all_gather(own_panel, PROW, axis=0, tiled=True)

    dinv_cols = lax.dynamic_slice_in_dim(dinv, col * x_rows, x_rows, 1)
    head = dot(panel_t, h_local[:, :width], ((0,), (0,))) + dot(dinv_cols, h_side[:, :width], ((1,), (0,)))
    rest = dot(panel_t, h_local[:, width:], ((0,), (0,))) + dot(dinv_cols, h_side[:, width:], ((1,), (0,)))
    x_head = exchange(head.reshape(n_col, x_rows, width), PCOL).sum(axis=0)

    octets = x_rows // 8
    tiles = x_head.reshape(octets, 8, n_blocks, nb).transpose(2, 0, 1, 3)
    tiles = exchange(tiles.reshape(n_blocks * octets, 8, nb), PROW)
    tiles = exchange(tiles, PCOL)
    x_cols = lax.all_gather(tiles.reshape(1, n_col * 8, nb), PROW, axis=0, tiled=True)
    x_cols = x_cols.reshape(n_blocks, octets * n_col * 8, nb)

    x_rest = exchange(rest.reshape(n_col, x_rows, width // 2), PCOL).sum(axis=0)
    tail = x_rest[:, :nb]
    dinv_tail = lax.dynamic_slice_in_dim(dinv, jnp.minimum(row, 1) * nb, nb, 1)
    tail_part = dot(dinv_tail, tail, ((1,), (1,)))
    tail_part = jnp.where(row < slab // nb, tail_part, 0.0)
    tail_part = exchange(tail_part.reshape(n_row, y_rows, x_rows), PROW).sum(axis=0)

    own_rows = lax.dynamic_slice_in_dim(panel_t, row * y_rows, y_rows, 1)
    x_cols = x_cols.transpose(1, 0, 2).reshape(slab, width)
    y_part = dot(x_cols, m_local, ((1,), (1,)))
    d_part = dot(x_cols, own_rows, ((1,), (0,)))
    both = jnp.concatenate([y_part, jnp.pad(d_part, ((0, 0), (0, 128 - y_rows)))], axis=1)
    both = both.reshape(octets, n_col, 8, -1).transpose(1, 0, 2, 3)
    both = exchange(both.reshape(n_col, x_rows, -1), PCOL).sum(axis=0)
    y_lead = both[:, :width].reshape(x_rows, n_blocks, 1, nb)
    y_diag = both[:, width : width + y_rows] + tail_part.T
    x_slab = jnp.concatenate([x_head, x_rest], axis=1).reshape(x_rows, h_blocks, 1, nb)
    return (x_slab, y_lead, y_diag)


def solution(mesh):
    grid = Mesh(mesh.devices.reshape(mesh.shape["prow"] // 2, 2, 4, mesh.shape["pcol"] // 4), AXES)
    return jax.shard_map(
        per_device,
        mesh=grid,
        in_specs=(
            P(None, PROW, None, None, PCOL, None),
            P(None, PCOL, None, None, PROW, None),
            P(PCOL, None, PROW, None),
            P(PCOL, None, PROW, None),
            P(),
        ),
        out_specs=(P(PCOL, None, PROW, None), P(PCOL, None, PROW, None), P(PCOL, PROW)),
        check_vma=False,
    )
```

```python
import functools

import jax
import jax.numpy as jnp
from jax import lax
from jax.experimental import pallas as pl
from jax.experimental.pallas import tpu as pltpu
from jax.sharding import Mesh, PartitionSpec as P

AXES = ("z", "core", "x", "y")
PROW = ("z", "core")
PCOL = ("x", "y")
F32, BF16 = jnp.float32, jnp.bfloat16


def shift(value, axis, by):
    size = lax.axis_size(axis)
    return lax.ppermute(value, axis, [(i, (i + by) % size) for i in range(size)])


def swap_core(value):
    return lax.ppermute(value, "core", [(0, 1), (1, 0)])


def pick(value, index, dim=0):
    return lax.dynamic_index_in_dim(value, index, dim, keepdims=False)


def ring_pairs(axis, first, second):
    size = lax.axis_size(axis)
    if AXES.index("core") < AXES.index(axis):
        names, at = ("core", axis), lambda k, i: k * size + i
    else:
        names, at = (axis, "core"), lambda k, i: i * 2 + k
    return names, [(at(k, i), at(k, (i + by) % size)) for k, by in enumerate((first, second)) for i in range(size)]


def core_first():
    return lax.axis_index("core") == 0


def line_gather(own):
    size = lax.axis_size("z")
    got = {0: own, size - 2: shift(own, "z", 2), 2: shift(own, "z", -2), size - 1: shift(own, "z", 1), 1: shift(own, "z", -1)}
    names, pairs = ring_pairs("z", 2, -2)
    got[4] = lax.ppermute(jnp.where(core_first(), got[size - 2], got[2]), names, pairs)
    got[size - 3] = shift(got[size - 2], "z", 1)
    got[3] = shift(got[2], "z", -1)
    return [part for d in range(size) for part in (got[d], swap_core(got[d]))]


def line_sum(piece):
    size = lax.axis_size("z")
    names, pairs = ring_pairs("z", 2, -2)
    far = lax.ppermute(piece(4), names, pairs)
    up = piece(2) + shift(piece(3), "z", 1) + jnp.where(core_first(), far, 0.0)
    down = piece(size - 2) + shift(piece(size - 3), "z", -1) + jnp.where(core_first(), 0.0, far)
    near = shift(piece(1), "z", 1) + shift(piece(size - 1), "z", -1)
    return piece(0) + near + shift(up, "z", 2) + shift(down, "z", -2)


def ring_sum(piece, axis):
    names, pairs = ring_pairs(axis, 1, -1)
    far = lax.ppermute(piece(2), names, pairs)
    up = piece(1) + jnp.where(core_first(), far, 0.0)
    down = piece(3) + jnp.where(core_first(), 0.0, far)
    return piece(0) + shift(up, axis, 1) + shift(down, axis, -1)


def near_sum(piece, axis):
    return piece(0) + shift(piece(2), axis, 2) + shift(piece(1), axis, 1) + shift(piece(3), axis, -1)


def torus_sum(parts):
    x, y = lax.axis_index("x"), lax.axis_index("y")
    half = parts.shape[1] // 2
    parts = parts.reshape(4, 4, *parts.shape[1:])
    first, second = parts[:, :, :half], parts[:, :, half:]
    middle = [ring_sum(lambda d: pick(first, (x + d) % 4, 0), "x"), ring_sum(lambda d: pick(second, (y + d) % 4, 1), "y")]
    sums = [near_sum(lambda d: pick(middle[0], (y + d) % 4), "y"), near_sum(lambda d: pick(middle[1], (x + d) % 4), "x")]
    return jnp.concatenate(sums)


def halves(value):
    high = value.astype(BF16)
    return high, (value - high.astype(F32)).astype(BF16)


def dot3(left, right, contract=((1,), (0,))):
    one = lambda a, b: lax.dot_general(a, b, (contract, ((), ())), preferred_element_type=F32)
    return one(left[0], right[0]) + (one(left[0], right[1]) + one(left[1], right[0]))


def call(kernel, out_shape, args, scratch=(), flops=0, spaces=(), name=None, limit=46):
    spaces = [*spaces, *[pltpu.VMEM] * (len(args) - len(spaces))]
    return pl.pallas_call(
        kernel,
        in_specs=[pl.BlockSpec(memory_space=space) for space in spaces],
        out_shape=out_shape,
        scratch_shapes=list(scratch),
        cost_estimate=pl.CostEstimate(flops=flops, bytes_accessed=2**22, transcendentals=0),
        compiler_params=pltpu.CompilerParams(vmem_limit_bytes=limit * 2**20),
        name=name,
    )(*args)


def blocks_kernel(n_tiles, rows, nb, *refs):
    flat_refs, out_ref = refs[:-1], refs[-1]
    first, per = 0, nb // 128
    for tiles, flat_ref in zip(n_tiles, flat_refs):
        for tile in range(tiles):
            at = pl.ds(tile % per * 128, 128)
            high, low = halves(flat_ref[pl.ds(tile, rows, stride=tiles), :])
            out_ref[0, first + tile // per, :, at], out_ref[1, first + tile // per, :, at] = high, low
        first += tiles // per


def as_blocks(parts, rows, nb, step=256):
    n_tiles = [part.size // rows // 128 for part in parts]
    count = sum(n_tiles) * 128 // nb
    return pl.pallas_call(
        functools.partial(blocks_kernel, n_tiles, step, nb),
        grid=(rows // step,),
        in_specs=[pl.BlockSpec((step * tiles, 128), lambda i: (i, 0)) for tiles in n_tiles],
        out_specs=pl.BlockSpec((2, count, step, nb), lambda i: (0, 0, i, 0)),
        out_shape=jax.ShapeDtypeStruct((2, count, rows, nb), BF16),
        cost_estimate=pl.CostEstimate(flops=10**8, bytes_accessed=2**24, transcendentals=0),
        compiler_params=pltpu.CompilerParams(vmem_limit_bytes=60 * 2**20),
        name="as_blocks",
    )(*[part.reshape(rows * tiles, 128) for part, tiles in zip(parts, n_tiles)])


def exact(left, right):
    return jnp.dot(left, right, precision=lax.Precision.HIGHEST, preferred_element_type=F32)


def invert_kernel(half, l_ref, out_ref, top_ref, bottom_ref):
    rows = lax.broadcasted_iota(jnp.int32, (half, half), 0)
    cols = lax.broadcasted_iota(jnp.int32, (half, half), 1)
    on_diag = rows == cols
    both = ((slice(0, half), top_ref), (slice(half, 2 * half), bottom_ref))
    for at, ref in both:
        ref[...] = jnp.where(on_diag, 1.0 / jnp.where(on_diag, l_ref[at, at], 1.0), 0.0)

    def level(step, _):
        row_block, col_block = rows >> step, cols >> step
        below = (row_block == col_block + 1) & ((row_block & 1) == 1)
        inverses = [ref[...] for _, ref in both]
        terms = [exact(jnp.where(below, l_ref[at, at], 0.0), inverse) for (at, _), inverse in zip(both, inverses)]
        for (_, ref), inverse, term in zip(both, inverses, terms):
            ref[...] = inverse - exact(inverse, term)
        return 0

    lax.fori_loop(0, half.bit_length() - 1, level, 0)
    top, bottom = top_ref[...], bottom_ref[...]
    out_ref[:half, :half] = top
    out_ref[:half, half:] = jnp.zeros((half, half), F32)
    out_ref[half:, :half] = -exact(bottom, exact(l_ref[half:, :half], top))
    out_ref[half:, half:] = bottom


def invert_diag(l_diag):
    half = l_diag.shape[0] // 2
    return call(
        functools.partial(invert_kernel, half),
        jax.ShapeDtypeStruct(l_diag.shape, F32),
        [l_diag],
        scratch=[pltpu.VMEM((half, half), F32)] * 2,
        flops=10**9,
        name="invert_diag",
        limit=16,
    )


def assemble(table_ref, refs, high_ref, low_ref):
    for n, ref in enumerate(refs):
        chunk = ref.shape[0]
        place = pl.ds(pl.multiple_of(table_ref[n] * chunk, chunk), chunk)
        high_ref[place, :], low_ref[place, :] = halves(ref[...])


def fetch_lower(blocks_ref, high_ref, low_ref, sems, order):
    nb, moves = blocks_ref.shape[3], {}
    for c in order:
        below, at = pl.ds(c * nb, high_ref.shape[0] - c * nb), pl.ds(c * nb, nb)
        moves[c] = [
            pltpu.make_async_copy(blocks_ref.at[half, c, below, :], ref.at[below, at], sems.at[c, half])
            for half, ref in enumerate((high_ref, low_ref))
        ]
        for move in moves[c]:
            move.start()
    return moves


def panel_kernel(side_ref, blocks_ref, p_ref, dinv_ref, sent_ref, kept_ref, m_high, m_low, p_high, p_low, f_high, f_low, sems):
    nb, width, rows = blocks_ref.shape[3], sent_ref.shape[1], sent_ref.shape[0]
    order = range(width // nb - 1, -1, -1)
    moves = fetch_lower(blocks_ref, m_high, m_low, sems, order)
    dinv = halves(dinv_ref[...])
    p_high[...], p_low[...] = halves(p_ref[...])
    for c in order:
        at = slice(c * nb, (c + 1) * nb)
        f_high[:, at], f_low[:, at] = halves(dot3(dinv, (p_high[:, at], p_low[:, at])))
    for c in order:
        for move in moves[c]:
            move.wait()
        at, below = slice(c * nb, (c + 1) * nb), slice(c * nb, width)
        product = -dot3((f_high[:, below], f_low[:, below]), (m_high[below, at], m_low[below, at]))
        sent_ref[:, at], kept_ref[:, at] = product[:rows], product[rows:]


def x_kernel(n, first, table_ref, *refs):
    refs, (blocks_ref, side_ref, out_ref, h_ref, high, low, h_sems) = refs[:n], refs[n:]
    nb, moves = blocks_ref.shape[3], []
    for c in range(out_ref.shape[1] // nb):
        moves.append([pltpu.make_async_copy(blocks_ref.at[i, first + c], h_ref.at[i, c], h_sems.at[c, i]) for i in range(2)])
        for move in moves[-1]:
            move.start()
    assemble(table_ref, refs, high, low)
    for c, pair in enumerate(moves):
        for move in pair:
            move.wait()
        at = slice(c * nb, (c + 1) * nb)
        out_ref[:, at] = side_ref[:, at] + dot3((high[...], low[...]), (h_ref[0, c], h_ref[1, c]))


def y_kernel(n, table_ref, *refs):
    refs, (blocks_ref, last_ref, out_ref, m_high, m_low, high, low, m_sems) = refs[:n], refs[n:]
    nb, width, rows = blocks_ref.shape[3], m_high.shape[0], last_ref.shape[0]
    order = range(width // nb)
    moves = fetch_lower(blocks_ref, m_high, m_low, m_sems, order)
    assemble(table_ref, refs, high, low)
    rhs = ((1,), (1,))
    out_ref[:, width:] = jnp.zeros((out_ref.shape[0], out_ref.shape[1] - width), F32)
    out_ref[:, width : width + rows] = dot3((high[...], low[...]), halves(last_ref[...]), rhs)
    for r in order:
        for move in moves[r]:
            move.wait()
        at, before = slice(r * nb, (r + 1) * nb), slice(0, (r + 1) * nb)
        out_ref[:, at] = dot3((high[:, before], low[:, before]), (m_high[at, before], m_low[at, before]), rhs)


def turned():
    pairs = []
    for r in range(16):
        for c in range(16):
            j = 2 * ((c // 2 - r // 2) % 8) + (r + c) % 2
            pairs.append((r * 16 + c, j * 16 + r))
    return pairs


def per_device(inv_lead, h_lead, h_slab, l_panel, l_diag):
    slab = l_diag.shape[0]
    n_blocks, nb = l_panel.shape[1], l_panel.shape[3]
    h_blocks = h_slab.shape[1]
    rows = l_panel.shape[0]
    n_z, n_core = lax.axis_size("z"), lax.axis_size("core")
    n_row = n_z * n_core
    n_col = lax.axis_size("x") * lax.axis_size("y")
    core, z = lax.axis_index("core"), lax.axis_index("z")
    x, y = lax.axis_index("x"), lax.axis_index("y")
    row, col = lax.axis_index(PROW), lax.axis_index(PCOL)
    width = n_blocks * nb
    y_rows = slab // n_row
    head = width + nb
    m_space = [pltpu.VMEM((width, width), BF16)] * 2
    sems = pltpu.SemaphoreType.DMA
    grid_of = lambda wide, kind: pltpu.VMEM((slab, wide), kind)

    own_p = l_panel.reshape(rows, width)
    p_rows = lax.all_to_all(jnp.broadcast_to(own_p, (n_col, *own_p.shape)), PCOL, split_axis=0, concat_axis=0, tiled=True)
    dinv = invert_diag(l_diag)
    blocks = as_blocks([inv_lead, h_lead], width, nb)
    h_side = h_slab.reshape(rows, h_blocks * nb)
    dinv_cols = lax.dynamic_slice_in_dim(dinv, col * rows, rows, 1)
    side = jnp.dot(dinv_cols, h_side, precision=lax.Precision.HIGH, preferred_element_type=F32)

    by_core = dinv.reshape(n_z, n_core, y_rows, slab)
    dinv_rows = jnp.concatenate([pick(by_core, 1 - core, 1), pick(by_core, core, 1)]).reshape(slab, slab)
    sent, kept = call(
        panel_kernel,
        [jax.ShapeDtypeStruct((slab // 2, width), F32)] * 2,
        [side, blocks, p_rows.reshape(slab, width), dinv_rows],
        spaces=[pl.ANY, pl.ANY],
        scratch=[*m_space, *[grid_of(width, BF16)] * 4, sems((n_blocks, 2))],
        flops=6 * slab * width * (slab + width),
        name="panel_part",
    )
    met, kept = swap_core(sent).reshape(n_z, y_rows, width), kept.reshape(n_z, y_rows, width)
    own_panel = line_sum(lambda d: pick(kept, (z + d) % n_z) + pick(met, (z + d) % n_z))

    panel_parts = line_gather(own_panel)
    places = [2 * ((z + d) % n_z) + (core + other) % 2 for d in range(n_z) for other in range(2)]
    panel_table = jnp.stack(places).astype(jnp.int32)
    wide = h_blocks * nb
    x_part = call(
        functools.partial(x_kernel, len(panel_parts), n_blocks),
        jax.ShapeDtypeStruct((slab, wide), F32),
        [panel_table, *panel_parts, blocks, side],
        spaces=[pltpu.SMEM, *[pltpu.VMEM] * len(panel_parts), pl.ANY],
        scratch=[
            pltpu.VMEM((2, h_blocks, width, nb), BF16),
            *[grid_of(width, BF16)] * 2,
            sems((h_blocks, 2)),
        ],
        flops=6 * slab * width * wide,
        name="x_part",
    )
    x_own = torus_sum(x_part.reshape(n_col, rows, wide))
    turned_x = lax.ppermute(x_own[:, :head], AXES, turned())

    x_parts = line_gather(turned_x)
    places = []
    for d in range(n_z):
        for other in range(2):
            places.append(2 * ((z + d + col // 2) % n_z) + (core + other + col) % 2)
    x_table = jnp.stack(places).astype(jnp.int32)
    dinv_part = lax.dynamic_slice(dinv, (row * y_rows, jnp.minimum(col, 1) * nb), (y_rows, nb))
    last_rows = jnp.concatenate([own_panel, jnp.where(col < slab // nb, dinv_part, 0.0)], axis=1)
    wide = width + 128
    y_part = call(
        functools.partial(y_kernel, len(x_parts)),
        jax.ShapeDtypeStruct((slab, wide), F32),
        [x_table, *x_parts, blocks, last_rows],
        spaces=[pltpu.SMEM, *[pltpu.VMEM] * len(x_parts), pl.ANY],
        scratch=[*m_space, *[grid_of(head, BF16)] * 2, sems((n_blocks, 2))],
        flops=6 * slab * width * wide,
        name="y_part",
    )
    y_sum = torus_sum(y_part.reshape(n_col, rows, wide))
    y_lead = y_sum[:, :width].reshape(rows, n_blocks, 1, nb)
    y_diag = y_sum[:, width : width + y_rows]
    x_slab = x_own.reshape(rows, h_blocks, 1, nb)
    return (x_slab, y_lead, y_diag)


def solution(mesh):
    grid = Mesh(mesh.devices.reshape(8, 2, 4, 4), AXES)
    return jax.shard_map(
        per_device,
        mesh=grid,
        in_specs=(
            P(None, PROW, None, None, PCOL, None),
            P(None, PCOL, None, None, PROW, None),
            P(PCOL, None, PROW, None),
            P(PCOL, None, PROW, None),
            P(),
        ),
        out_specs=(P(PCOL, None, PROW, None), P(PCOL, None, PROW, None), P(PCOL, PROW)),
        check_vma=False,
    )
```

```python
import functools

import jax
import jax.numpy as jnp
from jax import lax
from jax.experimental import pallas as pl
from jax.experimental.pallas import tpu as pltpu
from jax.sharding import Mesh, PartitionSpec as P

AXES = ("z", "core", "x", "y")
PROW = ("z", "core")
PCOL = ("x", "y")
F32, BF16 = jnp.float32, jnp.bfloat16


def shift(value, axis, by):
    size = lax.axis_size(axis)
    return lax.ppermute(value, axis, [(i, (i + by) % size) for i in range(size)])


def swap_core(value):
    return lax.ppermute(value, "core", [(0, 1), (1, 0)])


def pick(value, index, dim=0):
    return lax.dynamic_index_in_dim(value, index, dim, keepdims=False)


def ring_pairs(axis, first, second):
    size = lax.axis_size(axis)
    if AXES.index("core") < AXES.index(axis):
        names, at = ("core", axis), lambda k, i: k * size + i
    else:
        names, at = (axis, "core"), lambda k, i: i * 2 + k
    return names, [(at(k, i), at(k, (i + by) % size)) for k, by in enumerate((first, second)) for i in range(size)]


def core_first():
    return lax.axis_index("core") == 0


def line_gather(own, name):
    size = lax.axis_size("z")
    got = {0: own, 2: shift(own, "z", -2), size - 1: shift(own, "z", 1), 1: shift(own, "z", -1)}
    with jax.named_scope(name):
        got[size - 2] = shift(own, "z", 2)
    names, pairs = ring_pairs("z", 2, -2)
    got[4] = lax.ppermute(jnp.where(core_first(), got[size - 2], got[2]), names, pairs)
    got[size - 3] = shift(got[size - 2], "z", 1)
    got[3] = shift(got[2], "z", -1)
    return [part for d in range(size) for part in (got[d], swap_core(got[d]))]


def line_sum(piece):
    size = lax.axis_size("z")
    names, pairs = ring_pairs("z", 2, -2)
    far = lax.ppermute(piece(4), names, pairs)
    up = piece(2) + shift(piece(3), "z", 1) + jnp.where(core_first(), far, 0.0)
    down = piece(size - 2) + shift(piece(size - 3), "z", -1) + jnp.where(core_first(), 0.0, far)
    near = shift(piece(1), "z", 1) + shift(piece(size - 1), "z", -1)
    return piece(0) + near + shift(up, "z", 2) + shift(down, "z", -2)


def ring_sum(piece, axis):
    names, pairs = ring_pairs(axis, 1, -1)
    far = lax.ppermute(piece(2), names, pairs)
    up = piece(1) + jnp.where(core_first(), far, 0.0)
    down = piece(3) + jnp.where(core_first(), 0.0, far)
    return piece(0) + shift(up, axis, 1) + shift(down, axis, -1)


def near_sum(piece, axis):
    return piece(0) + shift(piece(2), axis, 2) + shift(piece(1), axis, 1) + shift(piece(3), axis, -1)


def torus_sum(parts):
    x, y = lax.axis_index("x"), lax.axis_index("y")
    half = parts.shape[1] // 2
    parts = parts.reshape(4, 4, *parts.shape[1:])
    first, second = parts[:, :, :half], parts[:, :, half:]
    middle = [ring_sum(lambda d: pick(first, (x + d) % 4, 0), "x"), ring_sum(lambda d: pick(second, (y + d) % 4, 1), "y")]
    sums = [near_sum(lambda d: pick(middle[0], (y + d) % 4), "y"), near_sum(lambda d: pick(middle[1], (x + d) % 4), "x")]
    return jnp.concatenate(sums)


def halves(value):
    high = value.astype(BF16)
    return high, (value - high.astype(F32)).astype(BF16)


def dot3(left, right, contract=((1,), (0,))):
    one = lambda a, b: lax.dot_general(a, b, (contract, ((), ())), preferred_element_type=F32)
    return one(left[0], right[0]) + (one(left[0], right[1]) + one(left[1], right[0]))


def call(kernel, out_shape, args, scratch=(), flops=0, spaces=(), name=None, limit=46):
    spaces = [*spaces, *[pltpu.VMEM] * (len(args) - len(spaces))]
    return pl.pallas_call(
        kernel,
        in_specs=[pl.BlockSpec(memory_space=space) for space in spaces],
        out_shape=out_shape,
        scratch_shapes=list(scratch),
        cost_estimate=pl.CostEstimate(flops=flops, bytes_accessed=2**22, transcendentals=0),
        compiler_params=pltpu.CompilerParams(vmem_limit_bytes=limit * 2**20),
        name=name,
    )(*args)


def blocks_kernel(n_tiles, rows, nb, *refs):
    flat_refs, out_ref = refs[:-1], refs[-1]
    first, per = 0, nb // 128
    for tiles, flat_ref in zip(n_tiles, flat_refs):
        for tile in range(tiles):
            at = pl.ds(tile % per * 128, 128)
            high, low = halves(flat_ref[pl.ds(tile, rows, stride=tiles), :])
            out_ref[0, first + tile // per, :, at], out_ref[1, first + tile // per, :, at] = high, low
        first += tiles // per


def as_blocks(parts, rows, nb, step=256):
    n_tiles = [part.size // rows // 128 for part in parts]
    count = sum(n_tiles) * 128 // nb
    return pl.pallas_call(
        functools.partial(blocks_kernel, n_tiles, step, nb),
        grid=(rows // step,),
        in_specs=[pl.BlockSpec((step * tiles, 128), lambda i: (i, 0)) for tiles in n_tiles],
        out_specs=pl.BlockSpec((2, count, step, nb), lambda i: (0, 0, i, 0)),
        out_shape=jax.ShapeDtypeStruct((2, count, rows, nb), BF16),
        cost_estimate=pl.CostEstimate(flops=10**8, bytes_accessed=2**24, transcendentals=0),
        compiler_params=pltpu.CompilerParams(vmem_limit_bytes=60 * 2**20),
        name="as_blocks",
    )(*[part.reshape(rows * tiles, 128) for part, tiles in zip(parts, n_tiles)])


def exact(left, right):
    return jnp.dot(left, right, precision=lax.Precision.HIGHEST, preferred_element_type=F32)


def invert_kernel(half, l_ref, out_ref, top_ref, bottom_ref):
    rows = lax.broadcasted_iota(jnp.int32, (half, half), 0)
    cols = lax.broadcasted_iota(jnp.int32, (half, half), 1)
    on_diag = rows == cols
    both = ((slice(0, half), top_ref), (slice(half, 2 * half), bottom_ref))
    for at, ref in both:
        ref[...] = jnp.where(on_diag, 1.0 / jnp.where(on_diag, l_ref[at, at], 1.0), 0.0)

    def level(step, _):
        row_block, col_block = rows >> step, cols >> step
        below = (row_block == col_block + 1) & ((row_block & 1) == 1)
        inverses = [ref[...] for _, ref in both]
        terms = [exact(jnp.where(below, l_ref[at, at], 0.0), inverse) for (at, _), inverse in zip(both, inverses)]
        for (_, ref), inverse, term in zip(both, inverses, terms):
            ref[...] = inverse - exact(inverse, term)
        return 0

    lax.fori_loop(0, half.bit_length() - 1, level, 0)
    top, bottom = top_ref[...], bottom_ref[...]
    out_ref[:half, :half] = top
    out_ref[:half, half:] = jnp.zeros((half, half), F32)
    out_ref[half:, :half] = -exact(bottom, exact(l_ref[half:, :half], top))
    out_ref[half:, half:] = bottom


def invert_diag(l_diag):
    half = l_diag.shape[0] // 2
    return call(
        functools.partial(invert_kernel, half),
        jax.ShapeDtypeStruct(l_diag.shape, F32),
        [l_diag],
        scratch=[pltpu.VMEM((half, half), F32)] * 2,
        flops=10**9,
        name="invert_diag",
        limit=16,
    )


def assemble(table_ref, refs, high_ref, low_ref):
    chunk, n = refs[0].shape[0], 0
    for ref in refs:
        for i in range(0, ref.shape[0], chunk):
            place = pl.ds(pl.multiple_of(table_ref[n] * chunk, chunk), chunk)
            high_ref[place, :], low_ref[place, :] = halves(ref[i : i + chunk, :])
            n += 1


def load_kernel(first, blocks_ref, after_ref, out_ref, sems):
    count = out_ref.shape[1]
    moves = [pltpu.make_async_copy(blocks_ref.at[i, first + c], out_ref.at[i, c], sems.at[c, i]) for c in range(count) for i in range(2)]
    for move in moves:
        move.start()
    for move in moves:
        move.wait()


def load_lower_kernel(blocks_ref, after_ref, high_ref, low_ref, sems):
    order = range(high_ref.shape[0] // blocks_ref.shape[3])
    moves = fetch_lower(blocks_ref, high_ref, low_ref, sems, order)
    for c in order:
        for move in moves[c]:
            move.wait()


def fetch_lower(blocks_ref, high_ref, low_ref, sems, order):
    nb, moves = blocks_ref.shape[3], {}
    for c in order:
        below, at = pl.ds(c * nb, high_ref.shape[0] - c * nb), pl.ds(c * nb, nb)
        moves[c] = [
            pltpu.make_async_copy(blocks_ref.at[half, c, below, :], ref.at[below, at], sems.at[c, half])
            for half, ref in enumerate((high_ref, low_ref))
        ]
        for move in moves[c]:
            move.start()
    return moves


def panel_kernel(chunk, table_ref, blocks_ref, p_ref, dinv_ref, sent_ref, kept_ref, m_high, m_low, d_high, d_low, p_high, p_low, f_high, f_low, sems):
    nb, width, rows = blocks_ref.shape[3], sent_ref.shape[1], sent_ref.shape[0]
    order = range(width // nb - 1, -1, -1)
    moves = fetch_lower(blocks_ref, m_high, m_low, sems, order)
    for n in range(2 * rows // chunk):
        place = pl.ds(pl.multiple_of(table_ref[n] * chunk, chunk), chunk)
        at = slice(n * chunk, (n + 1) * chunk)
        d_high[at, :], d_low[at, :] = halves(dinv_ref[place, :])
    p_high[...], p_low[...] = halves(p_ref[...])
    for c in order:
        at = slice(c * nb, (c + 1) * nb)
        f_high[:, at], f_low[:, at] = halves(dot3((d_high[...], d_low[...]), (p_high[:, at], p_low[:, at])))
    for c in order:
        for move in moves[c]:
            move.wait()
        at, below = slice(c * nb, (c + 1) * nb), slice(c * nb, width)
        product = -dot3((f_high[:, below], f_low[:, below]), (m_high[below, at], m_low[below, at]))
        sent_ref[:, at], kept_ref[:, at] = product[:rows], product[rows:]


def x_kernel(n, table_ref, *refs):
    refs, (h_ref, dinv_ref, side_ref, out_ref, high, low) = refs[:n], refs[n:]
    nb = h_ref.shape[3]
    assemble(table_ref, refs, high, low)
    dinv = halves(dinv_ref[...])
    for c in range(out_ref.shape[1] // nb):
        at = slice(c * nb, (c + 1) * nb)
        out_ref[:, at] = dot3(dinv, halves(side_ref[:, at])) + dot3((high[...], low[...]), (h_ref[0, c], h_ref[1, c]))


def y_kernel(n, nb, table_ref, *refs):
    refs, (m_high, m_low, last_ref, out_ref, high, low) = refs[:n], refs[n:]
    width, rows = m_high.shape[0], last_ref.shape[0]
    assemble(table_ref, refs, high, low)
    rhs = ((1,), (1,))
    out_ref[:, width:] = jnp.zeros((out_ref.shape[0], out_ref.shape[1] - width), F32)
    out_ref[:, width : width + rows] = dot3((high[...], low[...]), halves(last_ref[...]), rhs)
    for r in range(0, width, nb):
        at, before = slice(r, r + nb), slice(0, r + nb)
        out_ref[:, at] = dot3((high[:, before], low[:, before]), (m_high[at, before], m_low[at, before]), rhs)


def turned():
    pairs = []
    for r in range(16):
        for c in range(16):
            j = 2 * ((c // 2 - r // 2) % 8) + (r + c) % 2
            pairs.append((r * 16 + c, j * 16 + r))
    return pairs


def per_device(inv_lead, h_lead, h_slab, l_panel, l_diag):
    slab = l_diag.shape[0]
    n_blocks, nb = l_panel.shape[1], l_panel.shape[3]
    h_blocks = h_slab.shape[1]
    rows = l_panel.shape[0]
    n_z, n_core = lax.axis_size("z"), lax.axis_size("core")
    n_row = n_z * n_core
    n_col = lax.axis_size("x") * lax.axis_size("y")
    core, z = lax.axis_index("core"), lax.axis_index("z")
    x, y = lax.axis_index("x"), lax.axis_index("y")
    row, col = lax.axis_index(PROW), lax.axis_index(PCOL)
    width = n_blocks * nb
    y_rows = slab // n_row
    head = width + nb
    m_space = [pltpu.VMEM((width, width), BF16)] * 2
    sems = pltpu.SemaphoreType.DMA
    grid_of = lambda wide, kind: pltpu.VMEM((slab, wide), kind)

    own_p = l_panel.reshape(rows, width)
    p_rows = lax.all_to_all(jnp.broadcast_to(own_p, (n_col, *own_p.shape)), PCOL, split_axis=0, concat_axis=0, tiled=True)
    dinv = invert_diag(l_diag)
    blocks = as_blocks([inv_lead, h_lead], width, nb)
    h_side = h_slab.reshape(rows, h_blocks * nb)
    dinv_cols = lax.dynamic_slice_in_dim(dinv, col * rows, rows, 1)

    row_table = jnp.stack([2 * i + (core + 1 - kept) % 2 for kept in range(2) for i in range(n_z)]).astype(jnp.int32)
    sent, kept = call(
        functools.partial(panel_kernel, y_rows),
        [jax.ShapeDtypeStruct((slab // 2, width), F32)] * 2,
        [row_table, blocks, p_rows.reshape(slab, width), dinv],
        spaces=[pltpu.SMEM, pl.ANY],
        scratch=[*m_space, *[grid_of(slab, BF16)] * 2, *[grid_of(width, BF16)] * 4, sems((n_blocks, 2))],
        flops=6 * slab * width * (slab + width),
        name="panel_part",
    )
    met, kept = swap_core(sent).reshape(n_z, y_rows, width), kept.reshape(n_z, y_rows, width)
    own_panel = line_sum(lambda d: pick(kept, (z + d) % n_z) + pick(met, (z + d) % n_z))

    h_parts = call(
        functools.partial(load_kernel, n_blocks),
        jax.ShapeDtypeStruct((2, h_blocks, width, nb), BF16),
        [blocks, own_panel],
        spaces=[pl.ANY, pl.ANY],
        scratch=[sems((h_blocks, 2))],
        flops=10**7,
        name="load_h",
    )
    panel_parts = line_gather(own_panel, "panel_step")
    places = [2 * ((z + d) % n_z) + (core + other) % 2 for d in range(n_z) for other in range(2)]
    panel_table = jnp.stack(places).astype(jnp.int32)
    wide = h_blocks * nb
    x_part = call(
        functools.partial(x_kernel, len(panel_parts)),
        jax.ShapeDtypeStruct((slab, wide), F32),
        [panel_table, *panel_parts, h_parts, dinv_cols, h_side],
        spaces=[pltpu.SMEM],
        scratch=[*[grid_of(width, BF16)] * 2],
        flops=6 * slab * width * wide,
        name="x_part",
        limit=16,
    )
    x_own = torus_sum(x_part.reshape(n_col, rows, wide))
    turned_x = lax.ppermute(x_own[:, :head], AXES, turned())

    m_high, m_low = call(
        load_lower_kernel,
        [jax.ShapeDtypeStruct((width, width), BF16)] * 2,
        [blocks, turned_x],
        spaces=[pl.ANY, pl.ANY],
        scratch=[sems((n_blocks, 2))],
        flops=10**7,
        name="load_m",
    )
    x_parts = line_gather(turned_x, "x_step")
    places = [2 * ((z + d + col // 2) % n_z) + (core + other + col) % 2 for d in range(n_z) for other in range(2)]
    x_table = jnp.stack(places).astype(jnp.int32)
    dinv_part = lax.dynamic_slice(dinv, (row * y_rows, jnp.minimum(col, 1) * nb), (y_rows, nb))
    last_rows = jnp.concatenate([own_panel, jnp.where(col < slab // nb, dinv_part, 0.0)], axis=1)
    wide = width + 128
    y_part = call(
        functools.partial(y_kernel, len(x_parts), nb),
        jax.ShapeDtypeStruct((slab, wide), F32),
        [x_table, *x_parts, m_high, m_low, last_rows],
        spaces=[pltpu.SMEM],
        scratch=[*[grid_of(head, BF16)] * 2],
        flops=6 * slab * width * wide,
        name="y_part",
        limit=16,
    )
    y_sum = torus_sum(y_part.reshape(n_col, rows, wide))
    y_lead = y_sum[:, :width].reshape(rows, n_blocks, 1, nb)
    y_diag = y_sum[:, width : width + y_rows]
    x_slab = x_own.reshape(rows, h_blocks, 1, nb)
    return (x_slab, y_lead, y_diag)


def solution(mesh):
    grid = Mesh(mesh.devices.reshape(8, 2, 4, 4), AXES)
    return jax.shard_map(
        per_device,
        mesh=grid,
        in_specs=(
            P(None, PROW, None, None, PCOL, None),
            P(None, PCOL, None, None, PROW, None),
            P(PCOL, None, PROW, None),
            P(PCOL, None, PROW, None),
            P(),
        ),
        out_specs=(P(PCOL, None, PROW, None), P(PCOL, None, PROW, None), P(PCOL, PROW)),
        check_vma=False,
    )
```

```python
import functools

import jax
import jax.numpy as jnp
from jax import lax
from jax.experimental import pallas as pl
from jax.experimental.pallas import tpu as pltpu
from jax.sharding import Mesh, PartitionSpec as P

AXES = ("z", "core", "x", "y")
PROW = ("z", "core")
PCOL = ("x", "y")
F32, BF16 = jnp.float32, jnp.bfloat16


def shift(value, axis, by):
    size = lax.axis_size(axis)
    return lax.ppermute(value, axis, [(i, (i + by) % size) for i in range(size)])


def swap_core(value):
    return lax.ppermute(value, "core", [(0, 1), (1, 0)])


def pick(value, index, dim=0):
    return lax.dynamic_index_in_dim(value, index, dim, keepdims=False)


def ring_pairs(axis, first, second):
    size = lax.axis_size(axis)
    if AXES.index("core") < AXES.index(axis):
        names, at = ("core", axis), lambda k, i: k * size + i
    else:
        names, at = (axis, "core"), lambda k, i: i * 2 + k
    return names, [(at(k, i), at(k, (i + by) % size)) for k, by in enumerate((first, second)) for i in range(size)]


def core_first():
    return lax.axis_index("core") == 0


def line_gather(own, name):
    size = lax.axis_size("z")
    got = {0: own, 2: shift(own, "z", -2), size - 1: shift(own, "z", 1), 1: shift(own, "z", -1)}
    with jax.named_scope(name):
        got[size - 2] = shift(own, "z", 2)
    names, pairs = ring_pairs("z", 2, -2)
    got[4] = lax.ppermute(jnp.where(core_first(), got[size - 2], got[2]), names, pairs)
    got[size - 3] = shift(got[size - 2], "z", 1)
    got[3] = shift(got[2], "z", -1)
    return [part for d in range(size) for part in (got[d], swap_core(got[d]))]


def line_sum(piece):
    size = lax.axis_size("z")
    names, pairs = ring_pairs("z", 2, -2)
    far = lax.ppermute(piece(4), names, pairs)
    up = piece(2) + shift(piece(3), "z", 1) + jnp.where(core_first(), far, 0.0)
    down = piece(size - 2) + shift(piece(size - 3), "z", -1) + jnp.where(core_first(), 0.0, far)
    near = shift(piece(1), "z", 1) + shift(piece(size - 1), "z", -1)
    return piece(0) + near + shift(up, "z", 2) + shift(down, "z", -2)


def ring_sum(piece, axis):
    names, pairs = ring_pairs(axis, 1, -1)
    far = lax.ppermute(piece(2), names, pairs)
    up = piece(1) + jnp.where(core_first(), far, 0.0)
    down = piece(3) + jnp.where(core_first(), 0.0, far)
    return piece(0) + shift(up, axis, 1) + shift(down, axis, -1)


def near_sum(piece, axis):
    return piece(0) + shift(piece(2), axis, 2) + shift(piece(1), axis, 1) + shift(piece(3), axis, -1)


def torus_sum(parts):
    x, y = lax.axis_index("x"), lax.axis_index("y")
    half = parts.shape[1] // 2
    parts = parts.reshape(4, 4, *parts.shape[1:])
    first, second = parts[:, :, :half], parts[:, :, half:]
    middle = [ring_sum(lambda d: pick(first, (x + d) % 4, 0), "x"), ring_sum(lambda d: pick(second, (y + d) % 4, 1), "y")]
    sums = [near_sum(lambda d: pick(middle[0], (y + d) % 4), "y"), near_sum(lambda d: pick(middle[1], (x + d) % 4), "x")]
    return jnp.concatenate(sums)


def halves(value):
    high = value.astype(BF16)
    return high, (value - high.astype(F32)).astype(BF16)


def dot3(left, right, contract=((1,), (0,))):
    one = lambda a, b: lax.dot_general(a, b, (contract, ((), ())), preferred_element_type=F32)
    return one(left[0], right[0]) + (one(left[0], right[1]) + one(left[1], right[0]))


def call(kernel, out_shape, args, scratch=(), flops=0, spaces=(), name=None, limit=46):
    spaces = [*spaces, *[pltpu.VMEM] * (len(args) - len(spaces))]
    return pl.pallas_call(
        kernel,
        in_specs=[pl.BlockSpec(memory_space=space) for space in spaces],
        out_shape=out_shape,
        scratch_shapes=list(scratch),
        cost_estimate=pl.CostEstimate(flops=flops, bytes_accessed=2**22, transcendentals=0),
        compiler_params=pltpu.CompilerParams(vmem_limit_bytes=limit * 2**20),
        name=name,
    )(*args)


def blocks_kernel(n_tiles, rows, nb, *refs):
    flat_refs, out_ref = refs[:-1], refs[-1]
    first, per = 0, nb // 128
    for tiles, flat_ref in zip(n_tiles, flat_refs):
        for tile in range(tiles):
            at = pl.ds(tile % per * 128, 128)
            high, low = halves(flat_ref[pl.ds(tile, rows, stride=tiles), :])
            out_ref[0, first + tile // per, :, at], out_ref[1, first + tile // per, :, at] = high, low
        first += tiles // per


def as_blocks(parts, rows, nb, step=256):
    n_tiles = [part.size // rows // 128 for part in parts]
    count = sum(n_tiles) * 128 // nb
    return pl.pallas_call(
        functools.partial(blocks_kernel, n_tiles, step, nb),
        grid=(rows // step,),
        in_specs=[pl.BlockSpec((step * tiles, 128), lambda i: (i, 0)) for tiles in n_tiles],
        out_specs=pl.BlockSpec((2, count, step, nb), lambda i: (0, 0, i, 0)),
        out_shape=jax.ShapeDtypeStruct((2, count, rows, nb), BF16),
        cost_estimate=pl.CostEstimate(flops=10**8, bytes_accessed=2**24, transcendentals=0),
        compiler_params=pltpu.CompilerParams(vmem_limit_bytes=60 * 2**20),
        name="as_blocks",
    )(*[part.reshape(rows * tiles, 128) for part, tiles in zip(parts, n_tiles)])


def exact(left, right):
    return jnp.dot(left, right, precision=lax.Precision.HIGHEST, preferred_element_type=F32)


def invert_kernel(half, l_ref, out_ref, top_ref, bottom_ref):
    rows = lax.broadcasted_iota(jnp.int32, (half, half), 0)
    cols = lax.broadcasted_iota(jnp.int32, (half, half), 1)
    on_diag = rows == cols
    both = ((slice(0, half), top_ref), (slice(half, 2 * half), bottom_ref))
    for at, ref in both:
        ref[...] = jnp.where(on_diag, 1.0 / jnp.where(on_diag, l_ref[at, at], 1.0), 0.0)

    def level(step, _):
        row_block, col_block = rows >> step, cols >> step
        below = (row_block == col_block + 1) & ((row_block & 1) == 1)
        inverses = [ref[...] for _, ref in both]
        terms = [exact(jnp.where(below, l_ref[at, at], 0.0), inverse) for (at, _), inverse in zip(both, inverses)]
        for (_, ref), inverse, term in zip(both, inverses, terms):
            ref[...] = inverse - exact(inverse, term)
        return 0

    lax.fori_loop(0, half.bit_length() - 1, level, 0)
    top, bottom = top_ref[...], bottom_ref[...]
    out_ref[:half, :half] = top
    out_ref[:half, half:] = jnp.zeros((half, half), F32)
    out_ref[half:, :half] = -exact(bottom, exact(l_ref[half:, :half], top))
    out_ref[half:, half:] = bottom


def invert_diag(l_diag):
    half = l_diag.shape[0] // 2
    return call(
        functools.partial(invert_kernel, half),
        jax.ShapeDtypeStruct(l_diag.shape, F32),
        [l_diag],
        scratch=[pltpu.VMEM((half, half), F32)] * 2,
        flops=10**9,
        name="invert_diag",
        limit=16,
    )


def assemble(table_ref, refs, high_ref, low_ref):
    chunk, n = refs[0].shape[0], 0
    for ref in refs:
        for i in range(0, ref.shape[0], chunk):
            place = pl.ds(pl.multiple_of(table_ref[n] * chunk, chunk), chunk)
            high_ref[place, :], low_ref[place, :] = halves(ref[i : i + chunk, :])
            n += 1


def load_kernel(first, blocks_ref, after_ref, out_ref, sems):
    count = out_ref.shape[1]
    moves = [pltpu.make_async_copy(blocks_ref.at[i, first + c], out_ref.at[i, c], sems.at[c, i]) for c in range(count) for i in range(2)]
    for move in moves:
        move.start()
    for move in moves:
        move.wait()


def load_lower_kernel(blocks_ref, after_ref, high_ref, low_ref, sems):
    order = range(high_ref.shape[0] // blocks_ref.shape[3])
    moves = fetch_lower(blocks_ref, high_ref, low_ref, sems, order)
    for c in order:
        for move in moves[c]:
            move.wait()


def fetch_lower(blocks_ref, high_ref, low_ref, sems, order):
    nb, moves = blocks_ref.shape[3], {}
    for c in order:
        below, at = pl.ds(c * nb, high_ref.shape[0] - c * nb), pl.ds(c * nb, nb)
        moves[c] = [
            pltpu.make_async_copy(blocks_ref.at[half, c, below, :], ref.at[below, at], sems.at[c, half])
            for half, ref in enumerate((high_ref, low_ref))
        ]
        for move in moves[c]:
            move.start()
    return moves


def panel_kernel(chunk, nb, table_ref, m_high, m_low, p_ref, dinv_ref, sent_ref, kept_ref, d_high, d_low, p_high, p_low, f_high, f_low):
    width, rows = sent_ref.shape[1], sent_ref.shape[0]
    order = range(width // nb)
    for n in range(2 * rows // chunk):
        place = pl.ds(pl.multiple_of(table_ref[n] * chunk, chunk), chunk)
        at = slice(n * chunk, (n + 1) * chunk)
        d_high[at, :], d_low[at, :] = halves(dinv_ref[place, :])
    p_high[...], p_low[...] = halves(p_ref[...])
    for c in order:
        at = slice(c * nb, (c + 1) * nb)
        f_high[:, at], f_low[:, at] = halves(dot3((d_high[...], d_low[...]), (p_high[:, at], p_low[:, at])))
    for c in order:
        at, below = slice(c * nb, (c + 1) * nb), slice(c * nb, width)
        product = -dot3((f_high[:, below], f_low[:, below]), (m_high[below, at], m_low[below, at]))
        sent_ref[:, at], kept_ref[:, at] = product[:rows], product[rows:]


def x_kernel(n, table_ref, *refs):
    refs, (h_ref, dinv_ref, side_ref, out_ref, high, low) = refs[:n], refs[n:]
    nb = h_ref.shape[3]
    assemble(table_ref, refs, high, low)
    dinv = halves(dinv_ref[...])
    for c in range(out_ref.shape[1] // nb):
        at = slice(c * nb, (c + 1) * nb)
        out_ref[:, at] = dot3(dinv, halves(side_ref[:, at])) + dot3((high[...], low[...]), (h_ref[0, c], h_ref[1, c]))


def y_kernel(n, nb, table_ref, *refs):
    refs, (m_high, m_low, last_ref, out_ref, high, low) = refs[:n], refs[n:]
    width, rows = m_high.shape[0], last_ref.shape[0]
    assemble(table_ref, refs, high, low)
    rhs = ((1,), (1,))
    out_ref[:, width:] = jnp.zeros((out_ref.shape[0], out_ref.shape[1] - width), F32)
    out_ref[:, width : width + rows] = dot3((high[...], low[...]), halves(last_ref[...]), rhs)
    for r in range(0, width, nb):
        at, before = slice(r, r + nb), slice(0, r + nb)
        out_ref[:, at] = dot3((high[:, before], low[:, before]), (m_high[at, before], m_low[at, before]), rhs)


def turned():
    pairs = []
    for r in range(16):
        for c in range(16):
            j = 2 * ((c // 2 - r // 2) % 8) + (r + c) % 2
            pairs.append((r * 16 + c, j * 16 + r))
    return pairs


def per_device(inv_lead, h_lead, h_slab, l_panel, l_diag):
    slab = l_diag.shape[0]
    n_blocks, nb = l_panel.shape[1], l_panel.shape[3]
    h_blocks = h_slab.shape[1]
    rows = l_panel.shape[0]
    n_z, n_core = lax.axis_size("z"), lax.axis_size("core")
    n_row = n_z * n_core
    n_col = lax.axis_size("x") * lax.axis_size("y")
    core, z = lax.axis_index("core"), lax.axis_index("z")
    x, y = lax.axis_index("x"), lax.axis_index("y")
    row, col = lax.axis_index(PROW), lax.axis_index(PCOL)
    width = n_blocks * nb
    y_rows = slab // n_row
    head = width + nb
    sems = pltpu.SemaphoreType.DMA
    grid_of = lambda wide, kind: pltpu.VMEM((slab, wide), kind)

    own_p = l_panel.reshape(rows, width)
    p_rows = lax.all_to_all(jnp.broadcast_to(own_p, (n_col, *own_p.shape)), PCOL, split_axis=0, concat_axis=0, tiled=True)
    dinv = invert_diag(l_diag)
    blocks = as_blocks([inv_lead, h_lead], width, nb)
    h_side = h_slab.reshape(rows, h_blocks * nb)
    dinv_cols = lax.dynamic_slice_in_dim(dinv, col * rows, rows, 1)


    def load_lower(after):
        return call(
            load_lower_kernel,
            [jax.ShapeDtypeStruct((width, width), BF16)] * 2,
            [blocks, after],
            spaces=[pl.ANY, pl.ANY],
            scratch=[sems((n_blocks, 2))],
            flops=10**7,
            name="load_m",
        )

    row_table = jnp.stack([2 * i + (core + 1 - kept) % 2 for kept in range(2) for i in range(n_z)]).astype(jnp.int32)
    sent, kept = call(
        functools.partial(panel_kernel, y_rows, nb),
        [jax.ShapeDtypeStruct((slab // 2, width), F32)] * 2,
        [row_table, *load_lower(p_rows), p_rows.reshape(slab, width), dinv],
        spaces=[pltpu.SMEM],
        scratch=[*[grid_of(slab, BF16)] * 2, *[grid_of(width, BF16)] * 4],
        flops=6 * slab * width * (slab + width),
        name="panel_part",
        limit=24,
    )
    met, kept = swap_core(sent).reshape(n_z, y_rows, width), kept.reshape(n_z, y_rows, width)
    own_panel = line_sum(lambda d: pick(kept, (z + d) % n_z) + pick(met, (z + d) % n_z))

    h_parts = call(
        functools.partial(load_kernel, n_blocks),
        jax.ShapeDtypeStruct((2, h_blocks, width, nb), BF16),
        [blocks, own_panel],
        spaces=[pl.ANY, pl.ANY],
        scratch=[sems((h_blocks, 2))],
        flops=10**7,
        name="load_h",
    )
    panel_parts = line_gather(own_panel, "panel_step")
    places = [2 * ((z + d) % n_z) + (core + other) % 2 for d in range(n_z) for other in range(2)]
    panel_table = jnp.stack(places).astype(jnp.int32)
    wide = h_blocks * nb
    x_part = call(
        functools.partial(x_kernel, len(panel_parts)),
        jax.ShapeDtypeStruct((slab, wide), F32),
        [panel_table, *panel_parts, h_parts, dinv_cols, h_side],
        spaces=[pltpu.SMEM],
        scratch=[*[grid_of(width, BF16)] * 2],
        flops=6 * slab * width * wide,
        name="x_part",
        limit=16,
    )
    x_own = torus_sum(x_part.reshape(n_col, rows, wide))
    turned_x = lax.ppermute(x_own[:, :head], AXES, turned())

    m_high, m_low = load_lower(turned_x)
    x_parts = line_gather(turned_x, "x_step")
    places = [2 * ((z + d + col // 2) % n_z) + (core + other + col) % 2 for d in range(n_z) for other in range(2)]
    x_table = jnp.stack(places).astype(jnp.int32)
    dinv_part = lax.dynamic_slice(dinv, (row * y_rows, jnp.minimum(col, 1) * nb), (y_rows, nb))
    last_rows = jnp.concatenate([own_panel, jnp.where(col < slab // nb, dinv_part, 0.0)], axis=1)
    wide = width + 128
    y_part = call(
        functools.partial(y_kernel, len(x_parts), nb),
        jax.ShapeDtypeStruct((slab, wide), F32),
        [x_table, *x_parts, m_high, m_low, last_rows],
        spaces=[pltpu.SMEM],
        scratch=[*[grid_of(head, BF16)] * 2],
        flops=6 * slab * width * wide,
        name="y_part",
        limit=16,
    )
    y_sum = torus_sum(y_part.reshape(n_col, rows, wide))
    y_lead = y_sum[:, :width].reshape(rows, n_blocks, 1, nb)
    y_diag = y_sum[:, width : width + y_rows]
    x_slab = x_own.reshape(rows, h_blocks, 1, nb)
    return (x_slab, y_lead, y_diag)


def solution(mesh):
    grid = Mesh(mesh.devices.reshape(8, 2, 4, 4), AXES)
    return jax.shard_map(
        per_device,
        mesh=grid,
        in_specs=(
            P(None, PROW, None, None, PCOL, None),
            P(None, PCOL, None, None, PROW, None),
            P(PCOL, None, PROW, None),
            P(PCOL, None, PROW, None),
            P(),
        ),
        out_specs=(P(PCOL, None, PROW, None), P(PCOL, None, PROW, None), P(PCOL, PROW)),
        check_vma=False,
    )
```
